16 devices in a mesh: dp: 4 (over y, z, core), sp: 4 (over x).
Axes of the slice: x: 4, y: 2, z: 1, core: 2. Of those that a mesh axis runs over, the one named last changes fastest.
The devices are a block of a 4x4x4 slice.
Arguments:
- q: bfloat16 [128, 40, 128], P('dp'), parts along dimension 0
- k: bfloat16 [128, 4096, 10, 128], P('dp', 'sp'), parts along dimension 0
- v: bfloat16 [128, 4096, 10, 128], P('dp', 'sp'), parts along dimension 0
Outputs:
- q: bfloat16 [128, 40, 128], P('dp'), parts along dimension 0
There are 4 independent parts. The reference program is written for one: setup_inputs(seed, part) draws one part's arguments, and reference() takes and returns one part's arrays. A program takes and returns all parts, laid end to end along the dimension named above; each array names one.
All inputs are finite; a program needn't handle non-finite values.
Results may differ from the reference program's by a relative error of at most 0.012.
Values are sent between devices in bfloat16 or wider.
A program may use at most 1.5 GiB of HBM per device.

```python
import jax
import jax.numpy as jnp

BATCH = 32
CACHE = 4096
HEADS = 40
KV_HEADS = 10
HEAD = 128


def setup_inputs(seed: int = 0, part: int = 0) -> dict:
    kq, kk, kv = (jax.random.fold_in(k, part) for k in jax.random.split(jax.random.key(seed), 3))
    return {
        "q": (3 * jax.random.normal(kq, (BATCH, HEADS, HEAD), jnp.float32)).astype(jnp.bfloat16),
        "k": jax.random.normal(kk, (BATCH, CACHE, KV_HEADS, HEAD), jnp.float32).astype(jnp.bfloat16),
        "v": jax.random.normal(kv, (BATCH, CACHE, KV_HEADS, HEAD), jnp.float32).astype(jnp.bfloat16),
    }


def einsum(form, a, b):
    return jnp.einsum(form, a.astype(jnp.float32), b.astype(jnp.float32))


def reference(q, k, v):
    grouped = q.reshape(BATCH, KV_HEADS, -1, HEAD)
    scores = einsum("bgsd,bugd->bgsu", grouped, k) * HEAD**-0.5
    weights = jax.nn.softmax(scores, -1).astype(jnp.bfloat16)
    return einsum("bgsu,bugd->bgsd", weights, v).astype(jnp.bfloat16).reshape(BATCH, HEADS, HEAD)
```

```python
import functools

import jax
import jax.numpy as jnp
from jax import lax
from jax.experimental import pallas as pl
from jax.experimental.pallas import tpu as pltpu
from jax.sharding import PartitionSpec as P

SLOTS = 4
GROUP = 4
LOG2E = 1.4426950408889634


def kernel(n, q_hbm, k_hbm, v_hbm, o_ref, qv, kbuf, vbuf, sbuf, parts, stats, q_sem, k_sem, v_sem, part_send, part_recv, stat_send, stat_recv):
    seqs, heads, head = q_hbm.shape
    kv_heads, tokens = k_hbm.shape[1:3]
    rep = heads // kv_heads
    pairs = kv_heads // 2
    rows = 2 * rep
    half = head // 2
    scale = head**-0.5 * LOG2E
    me = lax.axis_index("sp")

    def fetch_k(b, slot):
        return pltpu.make_async_copy(k_hbm.at[b], kbuf.at[slot], k_sem.at[slot])

    def fetch_v(b, slot):
        return pltpu.make_async_copy(v_hbm.at[b], vbuf.at[slot], v_sem.at[slot])

    fetch_q = pltpu.make_async_copy(q_hbm, qv, q_sem)
    fetch_q.start()
    for b in range(SLOTS):
        fetch_k(b, b).start()
        fetch_v(b, b).start()

    barrier = pltpu.get_barrier_semaphore()
    for d in range(1, n):
        pl.semaphore_signal(barrier, inc=1, device_id={"sp": lax.rem(me + d, n)}, device_id_type=pl.DeviceIdType.MESH)

    row = lax.broadcasted_iota(jnp.int32, (rows, head), 0)
    lane = lax.broadcasted_iota(jnp.int32, (rows, head), 1)
    first = row < rep

    def scores(b, slot, into):
        q = qv[b].astype(jnp.float32)
        for p in range(pairs):
            x = q[p * rows : (p + 1) * rows]
            both = jnp.concatenate([jnp.where(first, x, 0.0), jnp.where(first, 0.0, x)], 1).astype(jnp.bfloat16)
            keys = jnp.concatenate([kbuf[slot, 2 * p], kbuf[slot, 2 * p + 1]], 1)
            sbuf[into, p] = lax.dot_general(both, keys, (((1,), (1,)), ((), ())), preferred_element_type=jnp.float32)

    def values(b, slot, source):
        outs = []
        stat = jnp.zeros((rows, head), jnp.float32)
        for p in range(pairs):
            s = sbuf[source, p] * scale
            high = jnp.max(s, 1, keepdims=True)
            w = jnp.exp2(s - high)
            total = jnp.sum(w, 1, keepdims=True)
            vals = jnp.concatenate([vbuf[slot, 2 * p], vbuf[slot, 2 * p + 1]], 1)
            seen = jnp.dot(w.astype(jnp.bfloat16), vals, preferred_element_type=jnp.float32)
            outs.append(jnp.where(first, seen[:, :head], seen[:, head:]))
            stat = jnp.where(lane == p, high, stat)
            stat = jnp.where(lane == half + p, total, stat)
        parts[me, b] = jnp.concatenate(outs, 0).astype(jnp.bfloat16)
        stats[me, b] = stat

    def sends(d, g, start, count):
        to = {"sp": lax.rem(me + d, n)}
        span = pl.ds(start, count)
        return (
            pltpu.make_async_remote_copy(parts.at[me, span], parts.at[me, span], part_send.at[d - 1, g], part_recv.at[d - 1, g], device_id=to, device_id_type=pl.DeviceIdType.MESH),
            pltpu.make_async_remote_copy(stats.at[me, span], stats.at[me, span], stat_send.at[d - 1, g], stat_recv.at[d - 1, g], device_id=to, device_id_type=pl.DeviceIdType.MESH),
        )

    order = [d for d in (2, 1, 3) if d < n]

    def send(g, start, count):
        for d in order:
            for c in sends(d, g, start, count):
                c.start()

    def arrive(g, start, count):
        for d in range(1, n):
            for c in sends(d, g, start, count):
                c.wait_recv()
                c.wait_send()

    def combine(b):
        st = [stats[d, b] for d in range(n)]
        top = functools.reduce(jnp.maximum, st)
        w = [jnp.exp2(s - top) for s in st]
        total = sum(a * pltpu.roll(s, half, 1) for a, s in zip(w, st))
        w = [a / total for a in w]
        x = [parts[d, b].astype(jnp.float32) for d in range(n)]
        outs = []
        for p in range(pairs):
            outs.append(sum(w[d][:, p : p + 1] * x[d][p * rows : (p + 1) * rows] for d in range(n)))
        o_ref[b] = jnp.concatenate(outs, 0).astype(o_ref.dtype)

    fetch_q.wait()
    fetch_k(0, 0).wait()
    scores(0, 0, 0)
    pl.semaphore_wait(barrier, n - 1)

    def step(i, carry):
        slot = lax.rem(i, SLOTS)
        before = lax.rem(i - 1, SLOTS)

        @pl.when(lax.rem(i, GROUP) == 1)
        def _():
            g = i // GROUP

            @pl.when(g >= 1)
            def _():
                send(g - 1, (g - 1) * GROUP, GROUP)

            @pl.when(g >= 2)
            def _():
                arrive(g - 2, (g - 2) * GROUP, GROUP)

                def one(j, c):
                    combine((g - 2) * GROUP + j)
                    return c

                lax.fori_loop(0, GROUP, one, 0)

        fetch_v(i - 1, before).wait()
        fetch_k(i, slot).wait()
        scores(i, slot, lax.rem(i, 2))
        values(i - 1, before, lax.rem(i - 1, 2))

        @pl.when(i + SLOTS < seqs)
        def _():
            fetch_k(i + SLOTS, slot).start()

        @pl.when(i - 1 + SLOTS < seqs)
        def _():
            fetch_v(i - 1 + SLOTS, before).start()

        return carry

    fetch_k_again = fetch_k(SLOTS, 0)
    fetch_k_again.start()
    lax.fori_loop(1, seqs, step, 0)

    groups = seqs // GROUP
    last = seqs - 1
    send(groups - 1, last - GROUP + 1, GROUP - 1)
    fetch_v(last, last % SLOTS).wait()
    values(last, last % SLOTS, last % 2)
    send(groups, last, 1)
    arrive(groups - 2, (groups - 2) * GROUP, GROUP)
    lax.fori_loop(0, GROUP, lambda j, c: (combine((groups - 2) * GROUP + j), c)[1], 0)
    arrive(groups - 1, last - GROUP + 1, GROUP - 1)
    lax.fori_loop(0, GROUP - 1, lambda j, c: (combine(last - GROUP + 1 + j), c)[1], 0)
    arrive(groups, last, 1)
    combine(last)


def solution(mesh):
    n = mesh.shape["sp"]

    def step(q, k, v):
        seqs, heads, head = q.shape
        tokens, kv_heads = k.shape[1:3]
        k, v = (jnp.transpose(a, (0, 2, 1, 3)) for a in (k, v))
        groups = seqs // GROUP + 1
        rows = 2 * heads // kv_heads
        f32, dma = jnp.float32, pltpu.SemaphoreType.DMA
        return pl.pallas_call(
            functools.partial(kernel, n),
            out_shape=jax.ShapeDtypeStruct(q.shape, q.dtype),
            in_specs=[pl.BlockSpec(memory_space=pl.ANY)] * 3,
            out_specs=pl.BlockSpec(memory_space=pltpu.VMEM),
            scratch_shapes=[
                pltpu.VMEM(q.shape, q.dtype),
                pltpu.VMEM((SLOTS, kv_heads, tokens, head), k.dtype),
                pltpu.VMEM((SLOTS, kv_heads, tokens, head), v.dtype),
                pltpu.VMEM((2, kv_heads // 2, rows, tokens), f32),
                pltpu.VMEM((n, seqs, heads, head), jnp.bfloat16),
                pltpu.VMEM((n, seqs, rows, head), f32),
                dma,
                dma((SLOTS,)),
                dma((SLOTS,)),
                dma((n - 1, groups)),
                dma((n - 1, groups)),
                dma((n - 1, groups)),
                dma((n - 1, groups)),
            ],
            compiler_params=pltpu.CompilerParams(collective_id=0, has_side_effects=True, vmem_limit_bytes=60 * 2**20),
        )(q, k, v)

    return jax.shard_map(
        step,
        mesh=mesh,
        in_specs=(P("dp", None, None), P("dp", "sp", None, None), P("dp", "sp", None, None)),
        out_specs=P("dp", None, None),
        check_vma=False,
    )
```

```python
import functools

import jax
import jax.numpy as jnp
from jax import lax
from jax.experimental import pallas as pl
from jax.experimental.pallas import tpu as pltpu
from jax.sharding import PartitionSpec as P

SLOTS = 4
AHEAD = 6
TILE = 4
LOG2E = 1.4426950408889634
MESH = pl.DeviceIdType.MESH


def kernel(n, q_hbm, k_hbm, v_hbm, o_ref, qv, kbuf, vbuf, sbuf, wbuf, parts, stats, q_sem, k_sem, v_sem, end_sem, part_send, part_recv, stat_send, stat_recv):
    seqs, heads, head = q_hbm.shape
    kv_heads = k_hbm.shape[1]
    rep = heads // kv_heads
    pairs = kv_heads // 2
    rows = 2 * rep
    half = head // 2
    wide = half // TILE
    last = seqs - 1
    tiles = seqs // TILE
    old = tiles // 2
    early = (pairs - 1) * rows
    scale = head**-0.5 * LOG2E
    me = lax.axis_index("sp")
    groups = ((0, old * TILE), (old * TILE, last - TILE + 1), (last - TILE + 1, last))

    def fetch_k(b):
        slot = lax.rem(b, SLOTS)
        return pltpu.make_async_copy(k_hbm.at[b], kbuf.at[slot], k_sem.at[slot])

    def fetch_v(b):
        slot = lax.rem(b, SLOTS)
        return pltpu.make_async_copy(v_hbm.at[b], vbuf.at[slot], v_sem.at[slot])

    def fetch_end(e):
        cut = early // rep
        part = pl.ds(0, cut) if e == 0 else pl.ds(cut, kv_heads - cut)
        return pltpu.make_async_copy(v_hbm.at[last, part], vbuf.at[last % SLOTS, part], end_sem.at[e])

    def fetch_q():
        return pltpu.make_async_copy(q_hbm, qv, q_sem)

    fetch_q().start()
    barrier = pltpu.get_barrier_semaphore()
    for d in range(1, n):
        pl.semaphore_signal(barrier, inc=1, device_id={"sp": lax.rem(me + d, n)}, device_id_type=MESH)
    for b in range(SLOTS):
        fetch_k(b).start()

    first = lax.broadcasted_iota(jnp.int32, (rows, head), 0) < rep
    lane = lax.broadcasted_iota(jnp.int32, (rows, head), 1)

    def scores(b):
        q = qv[b].astype(jnp.float32)
        for p in range(pairs):
            x = q[p * rows : (p + 1) * rows]
            both = jnp.concatenate([jnp.where(first, x, 0.0), jnp.where(first, 0.0, x)], 1).astype(jnp.bfloat16)
            slot = lax.rem(b, SLOTS)
            keys = jnp.concatenate([kbuf[slot, 2 * p], kbuf[slot, 2 * p + 1]], 1)
            sbuf[lax.rem(b, 2), p] = lax.dot_general(both, keys, (((1,), (1,)), ((), ())), preferred_element_type=jnp.float32)

    def weights(b):
        tile = b // TILE
        at = lax.rem(b, TILE) * wide
        stat = stats[me, tile]
        for p in range(pairs):
            s = sbuf[lax.rem(b, 2), p] * scale
            high = jnp.max(s, 1, keepdims=True)
            w = jnp.exp2(s - high)
            total = jnp.sum(w, 1, keepdims=True)
            stat = jnp.where(lane == at + p, high, stat)
            stat = jnp.where(lane == half + at + p, total, stat)
            wbuf[lax.rem(b, AHEAD + 1), p] = w.astype(jnp.bfloat16)
        stats[me, tile] = stat

    def seen(b, p):
        slot = lax.rem(b, SLOTS)
        vals = jnp.concatenate([vbuf[slot, 2 * p], vbuf[slot, 2 * p + 1]], 1)
        out = jnp.dot(wbuf[lax.rem(b, AHEAD + 1), p], vals, preferred_element_type=jnp.float32)
        return jnp.where(first, out[:, :head], out[:, head:])

    def values(b):
        parts[me, b] = jnp.concatenate([seen(b, p) for p in range(pairs)], 0).astype(jnp.bfloat16)

    def to(d):
        return {"sp": lax.rem(me + d, n)}

    peers = sorted(range(1, n), key=lambda d: -min(d, n - d))

    def send(ref, sent, received):
        for d in peers:
            pltpu.make_async_remote_copy(ref, ref, sent.at[0], received, device_id=to(d), device_id_type=MESH).start()

    def send_part(b, g):
        send(parts.at[me, b], part_send, part_recv.at[g])

    def send_stat(t, g):
        send(stats.at[me, t], stat_send, stat_recv.at[g])

    def landed(ref, sem):
        pltpu.make_async_copy(ref, ref, sem).wait()

    others = pl.ds(0, n - 1)

    def shares(t):
        st = [stats[d, t] for d in range(n)]
        top = functools.reduce(jnp.maximum, st)
        w = [jnp.exp2(s - top) for s in st]
        total = sum(a * pltpu.roll(s, half, 1) for a, s in zip(w, st))
        return [a / total for a in w]

    def factors(w, j):
        lanes = [j * wide + p for p in range(pairs)]
        return [[jnp.broadcast_to(a[:, x : x + 1], (rows, head)) for a in w] for x in lanes]

    def mixed(b, ps, f):
        x = [parts[d, b, pl.ds(ps[0] * rows, len(ps) * rows)].astype(jnp.float32) for d in range(n)]
        return jnp.concatenate([sum(f[p][d] * x[d][i * rows : (i + 1) * rows] for d in range(n)) for i, p in enumerate(ps)], 0)

    def combine(t, w, j):
        o_ref[t * TILE + j] = mixed(t * TILE + j, range(pairs), factors(w, j)).astype(o_ref.dtype)

    def combine_tile(t, carry):
        w = shares(t)
        for j in range(TILE):
            combine(t, w, j)
        return carry

    def refill_k(b):
        @pl.when(b < seqs)
        def _():
            fetch_k(b).start()

    def refill_v(b):
        @pl.when((b >= 0) & (b < last))
        def _():
            fetch_v(b).start()

        @pl.when(b == last)
        def _():
            for e in range(2):
                fetch_end(e).start()

    fetch_q().wait()
    fetch_k(0).wait()
    scores(0)
    refill_k(SLOTS)

    def fill(i, carry):
        fetch_k(i).wait()
        weights(i - 1)
        scores(i)
        refill_k(i + SLOTS)
        refill_v(i - AHEAD + SLOTS)
        return carry

    lax.fori_loop(1, AHEAD, fill, 0)
    pl.semaphore_wait(barrier, n - 1)
    send_stat(0, 0)

    def group(b):
        return jnp.where(b < groups[1][0], 0, jnp.where(b < groups[2][0], 1, 2))

    def step(i, carry):
        done = i - AHEAD - 1

        @pl.when(done >= 0)
        def _():
            send_part(done, group(done))

        @pl.when((lax.rem(i, TILE) == 1) & (i >= AHEAD + 1))
        def _():
            t = i // TILE - 1
            send_stat(t, group(t * TILE))

        @pl.when(i == groups[0][1] + AHEAD + TILE)
        def _():
            span = pl.ds(0, groups[0][1])
            landed(parts.at[others, span], part_recv.at[0])
            landed(stats.at[others, pl.ds(0, old)], stat_recv.at[0])
            lax.fori_loop(0, old, combine_tile, 0)

        fetch_k(i).wait()
        fetch_v(i - AHEAD).wait()
        values(i - AHEAD)
        weights(i - 1)
        scores(i)
        refill_k(i + SLOTS)
        refill_v(i - AHEAD + SLOTS)
        return carry

    lax.fori_loop(AHEAD, seqs, step, 0)

    weights(last)
    send_stat(tiles - 1, 2)

    def finish(b, carry):
        fetch_v(b).wait()
        send_part(b - 1, group(b - 1))
        values(b)
        refill_v(b + SLOTS)
        return carry

    lax.fori_loop(last - AHEAD + 1, last, finish, 0)

    fetch_end(0).wait()
    send_part(last - 1, 2)
    parts[me, last, pl.ds(0, early)] = jnp.concatenate([seen(last, p) for p in range(pairs - 1)], 0).astype(jnp.bfloat16)
    fetch_end(1).wait()
    send(parts.at[me, last, pl.ds(0, early)], part_send, part_recv.at[3])
    parts[me, last, pl.ds(early, rows)] = seen(last, pairs - 1).astype(jnp.bfloat16)
    send(parts.at[me, last, pl.ds(early, rows)], part_send, part_recv.at[4])

    landed(parts.at[others, pl.ds(groups[1][0], groups[1][1] - groups[1][0])], part_recv.at[1])
    landed(stats.at[others, pl.ds(old, tiles - 1 - old)], stat_recv.at[1])
    lax.fori_loop(old, tiles - 1, combine_tile, 0)
    landed(stats.at[others, pl.ds(0, 1)], stat_recv.at[2])
    w = shares(tiles - 1)
    landed(parts.at[others, pl.ds(0, TILE - 1)], part_recv.at[2])
    for j in range(TILE - 1):
        combine(tiles - 1, w, j)
    f = factors(w, TILE - 1)
    landed(parts.at[others, last, pl.ds(0, early)], part_recv.at[3])
    o_ref[last, pl.ds(0, early)] = mixed(last, range(pairs - 1), f).astype(o_ref.dtype)
    landed(parts.at[others], part_send.at[0])
    landed(stats.at[others], stat_send.at[0])
    landed(parts.at[others, last, pl.ds(early, rows)], part_recv.at[4])
    o_ref[last, pl.ds(early, rows)] = mixed(last, [pairs - 1], f).astype(o_ref.dtype)


def solution(mesh):
    n = mesh.shape["sp"]

    def step(q, k, v):
        seqs, heads, head = q.shape
        tokens, kv_heads = k.shape[1:3]
        k, v = (jnp.transpose(a, (0, 2, 1, 3)) for a in (k, v))
        pairs, rows = kv_heads // 2, 2 * heads // kv_heads
        f32, bf16, dma = jnp.float32, jnp.bfloat16, pltpu.SemaphoreType.DMA
        return pl.pallas_call(
            functools.partial(kernel, n),
            out_shape=jax.ShapeDtypeStruct(q.shape, q.dtype),
            in_specs=[pl.BlockSpec(memory_space=pl.ANY)] * 3,
            out_specs=pl.BlockSpec(memory_space=pltpu.VMEM),
            scratch_shapes=[
                pltpu.VMEM(q.shape, q.dtype),
                pltpu.VMEM((SLOTS, kv_heads, tokens, head), k.dtype),
                pltpu.VMEM((SLOTS, kv_heads, tokens, head), v.dtype),
                pltpu.VMEM((2, pairs, rows, tokens), f32),
                pltpu.VMEM((AHEAD + 1, pairs, rows, tokens), bf16),
                pltpu.VMEM((n, seqs, heads, head), bf16),
                pltpu.VMEM((n, seqs // TILE, rows, head), f32),
                dma,
                dma((SLOTS,)),
                dma((SLOTS,)),
                dma((2,)),
                dma((1,)),
                dma((5,)),
                dma((1,)),
                dma((3,)),
            ],
            compiler_params=pltpu.CompilerParams(collective_id=0, has_side_effects=True, vmem_limit_bytes=32 * 2**20),
        )(*(pltpu.with_memory_space_constraint(a, pltpu.HBM) for a in (q, k, v)))

    return jax.shard_map(
        step,
        mesh=mesh,
        in_specs=(P("dp", None, None), P("dp", "sp", None, None), P("dp", "sp", None, None)),
        out_specs=P("dp", None, None),
        check_vma=False,
    )
```

```python
import functools

import jax
import jax.numpy as jnp
from jax import lax
from jax.experimental import pallas as pl
from jax.experimental.pallas import tpu as pltpu
from jax.sharding import PartitionSpec as P

SLOTS = 4
AHEAD = 6
TILE = 4
LOG2E = 1.4426950408889634
MESH = pl.DeviceIdType.MESH
dma = pltpu.SemaphoreType.DMA


def kernel(n, q_hbm, k_hbm, v_hbm, o_ref, qv, kbuf, vbuf, sbuf, wbuf, parts, stats, part_send, part_recv, stat_send, stat_recv):
    seqs, heads, head = q_hbm.shape
    kv_heads = k_hbm.shape[1]
    rep = heads // kv_heads
    pairs = kv_heads // 2
    rows = 2 * rep
    half = head // 2
    wide = half // TILE
    last = seqs - 1
    tiles = seqs // TILE
    old = tiles // 2
    ahead = pairs - 2
    early = ahead * rows
    scale = head**-0.5 * LOG2E
    me = lax.axis_index("sp")
    groups = ((0, old * TILE), (old * TILE, last - TILE + 1), (last - TILE + 1, last))

    first = lax.broadcasted_iota(jnp.int32, (rows, head), 0) < rep
    lane = lax.broadcasted_iota(jnp.int32, (rows, head), 1)

    def scores(b):
        q = qv[b].astype(jnp.float32)
        for p in range(pairs):
            x = q[p * rows : (p + 1) * rows]
            both = jnp.concatenate([jnp.where(first, x, 0.0), jnp.where(first, 0.0, x)], 1).astype(jnp.bfloat16)
            slot = lax.rem(b, SLOTS)
            keys = jnp.concatenate([kbuf[slot, 2 * p], kbuf[slot, 2 * p + 1]], 1)
            sbuf[lax.rem(b, 2), p] = lax.dot_general(both, keys, (((1,), (1,)), ((), ())), preferred_element_type=jnp.float32)

    def weights(b):
        tile = b // TILE
        at = lax.rem(b, TILE) * wide
        stat = stats[me, tile]
        for p in range(pairs):
            s = sbuf[lax.rem(b, 2), p] * scale
            high = jnp.max(s, 1, keepdims=True)
            w = jnp.exp2(s - high)
            total = jnp.sum(w, 1, keepdims=True)
            stat = jnp.where(lane == at + p, high, stat)
            stat = jnp.where(lane == half + at + p, total, stat)
            wbuf[lax.rem(b, AHEAD + 1), p] = w.astype(jnp.bfloat16)
        stats[me, tile] = stat

    def seen(b, p):
        slot = lax.rem(b, SLOTS)
        vals = jnp.concatenate([vbuf[slot, 2 * p], vbuf[slot, 2 * p + 1]], 1)
        out = jnp.dot(wbuf[lax.rem(b, AHEAD + 1), p], vals, preferred_element_type=jnp.float32)
        return jnp.where(first, out[:, :head], out[:, head:])

    def values(b):
        parts[me, b] = jnp.concatenate([seen(b, p) for p in range(pairs)], 0).astype(jnp.bfloat16)

    def to(d):
        return {"sp": lax.rem(me + d, n)}

    peers = sorted(range(1, n), key=lambda d: -min(d, n - d))

    def send(ref, sent, received):
        for d in peers:
            pltpu.make_async_remote_copy(ref, ref, sent.at[0], received, device_id=to(d), device_id_type=MESH).start()

    def send_part(b, g):
        send(parts.at[me, b], part_send, part_recv.at[g])

    def send_stat(t, g):
        send(stats.at[me, t], stat_send, stat_recv.at[g])

    def landed(ref, sem):
        pltpu.make_async_copy(ref, ref, sem).wait()

    others = pl.ds(0, n - 1)

    def shares(t):
        st = [stats[d, t] for d in range(n)]
        top = functools.reduce(jnp.maximum, st)
        w = [jnp.exp2(s - top) for s in st]
        total = sum(a * pltpu.roll(s, half, 1) for a, s in zip(w, st))
        return [a / total for a in w]

    def factors(w, j):
        lanes = [j * wide + p for p in range(pairs)]
        return [[jnp.broadcast_to(a[:, x : x + 1], (rows, head)) for a in w] for x in lanes]

    def mixed(b, ps, f):
        x = [parts[d, b, pl.ds(ps[0] * rows, len(ps) * rows)].astype(jnp.float32) for d in range(n)]
        return jnp.concatenate([sum(f[p][d] * x[d][i * rows : (i + 1) * rows] for d in range(n)) for i, p in enumerate(ps)], 0)

    def combine(t, w, j):
        o_ref[t * TILE + j] = mixed(t * TILE + j, range(pairs), factors(w, j)).astype(o_ref.dtype)

    def combine_tile(t, carry):
        w = shares(t)
        for j in range(TILE):
            combine(t, w, j)
        return carry

    @functools.partial(pl.run_scoped, q_sem=dma, k_sem=dma((SLOTS,)), v_sem=dma((SLOTS,)), end_sem=dma((2,)))
    def _(q_sem, k_sem, v_sem, end_sem):
        def fetch_k(b):
            slot = lax.rem(b, SLOTS)
            return pltpu.make_async_copy(k_hbm.at[b], kbuf.at[slot], k_sem.at[slot])

        def fetch_v(b):
            slot = lax.rem(b, SLOTS)
            return pltpu.make_async_copy(v_hbm.at[b], vbuf.at[slot], v_sem.at[slot])

        def fetch_end(e):
            cut = early // rep
            part = pl.ds(0, cut) if e == 0 else pl.ds(cut, kv_heads - cut)
            return pltpu.make_async_copy(v_hbm.at[last, part], vbuf.at[last % SLOTS, part], end_sem.at[e])

        def fetch_q():
            return pltpu.make_async_copy(q_hbm, qv, q_sem)

        fetch_q().start()
        barrier = pltpu.get_barrier_semaphore()
        for d in range(1, n):
            pl.semaphore_signal(barrier, inc=1, device_id={"sp": lax.rem(me + d, n)}, device_id_type=MESH)
        for b in range(SLOTS):
            fetch_k(b).start()

        def refill_k(b):
            @pl.when(b < seqs)
            def _():
                fetch_k(b).start()

        def refill_v(b):
            @pl.when((b >= 0) & (b < last))
            def _():
                fetch_v(b).start()

            @pl.when(b == last)
            def _():
                for e in range(2):
                    fetch_end(e).start()

        fetch_q().wait()
        fetch_k(0).wait()
        scores(0)
        refill_k(SLOTS)

        def fill(i, carry):
            fetch_k(i).wait()
            weights(i - 1)
            scores(i)
            refill_k(i + SLOTS)
            refill_v(i - AHEAD + SLOTS)
            return carry

        lax.fori_loop(1, AHEAD, fill, 0)
        pl.semaphore_wait(barrier, n - 1)
        send_stat(0, 0)

        def group(b):
            return jnp.where(b < groups[1][0], 0, jnp.where(b < groups[2][0], 1, 2))

        def step(i, carry):
            done = i - AHEAD - 1

            @pl.when(done >= 0)
            def _():
                send_part(done, group(done))

            @pl.when((lax.rem(i, TILE) == 1) & (i >= AHEAD + 1))
            def _():
                t = i // TILE - 1
                send_stat(t, jnp.minimum(group(t * TILE), 1))

            @pl.when(i == groups[0][1] + AHEAD + TILE)
            def _():
                span = pl.ds(0, groups[0][1])
                landed(parts.at[others, span], part_recv.at[0])
                landed(stats.at[others, pl.ds(0, old)], stat_recv.at[0])
                lax.fori_loop(0, old, combine_tile, 0)

            fetch_k(i).wait()
            fetch_v(i - AHEAD).wait()
            values(i - AHEAD)
            weights(i - 1)
            scores(i)
            refill_k(i + SLOTS)
            refill_v(i - AHEAD + SLOTS)
            return carry

        lax.fori_loop(AHEAD, seqs, step, 0)

        weights(last)
        send_stat(tiles - 1, 1)

        def finish(b, carry):
            fetch_v(b).wait()
            send_part(b - 1, group(b - 1))
            values(b)
            refill_v(b + SLOTS)
            return carry

        lax.fori_loop(last - AHEAD + 1, last, finish, 0)

        fetch_end(0).wait()
        send_part(last - 1, 2)
        outs = [seen(last, p) for p in range(ahead)]
        fetch_end(1).wait()
        parts[me, last, pl.ds(0, early)] = jnp.concatenate(outs, 0).astype(jnp.bfloat16)
        outs = [seen(last, p) for p in range(ahead, pairs)]
        parts[me, last, pl.ds(early, heads - early)] = jnp.concatenate(outs, 0).astype(jnp.bfloat16)
        send(parts.at[me, last], part_send, part_recv.at[3])

    landed(parts.at[others, pl.ds(groups[1][0], groups[1][1] - groups[1][0])], part_recv.at[1])
    landed(stats.at[others, pl.ds(old, tiles - old)], stat_recv.at[1])
    lax.fori_loop(old, tiles - 1, combine_tile, 0)
    w = shares(tiles - 1)
    landed(parts.at[others, pl.ds(0, TILE - 1)], part_recv.at[2])
    for j in range(TILE - 1):
        combine(tiles - 1, w, j)
    f = factors(w, TILE - 1)
    landed(parts.at[others], part_send.at[0])
    landed(stats.at[others], stat_send.at[0])
    landed(parts.at[others, last], part_recv.at[3])
    o_ref[last] = mixed(last, range(pairs), f).astype(o_ref.dtype)


def solution(mesh):
    n = mesh.shape["sp"]

    def step(q, k, v):
        seqs, heads, head = q.shape
        tokens, kv_heads = k.shape[1:3]
        k, v = (jnp.transpose(a, (0, 2, 1, 3)) for a in (k, v))
        pairs, rows = kv_heads // 2, 2 * heads // kv_heads
        f32, bf16 = jnp.float32, jnp.bfloat16
        return pl.pallas_call(
            functools.partial(kernel, n),
            out_shape=jax.ShapeDtypeStruct(q.shape, q.dtype),
            in_specs=[pl.BlockSpec(memory_space=pl.ANY)] * 3,
            out_specs=pl.BlockSpec(memory_space=pltpu.VMEM),
            scratch_shapes=[
                pltpu.VMEM(q.shape, q.dtype),
                pltpu.VMEM((SLOTS, kv_heads, tokens, head), k.dtype),
                pltpu.VMEM((SLOTS, kv_heads, tokens, head), v.dtype),
                pltpu.VMEM((2, pairs, rows, tokens), f32),
                pltpu.VMEM((AHEAD + 1, pairs, rows, tokens), bf16),
                pltpu.VMEM((n, seqs, heads, head), bf16),
                pltpu.VMEM((n, seqs // TILE, rows, head), f32),
                dma((1,)),
                dma((4,)),
                dma((1,)),
                dma((2,)),
            ],
            compiler_params=pltpu.CompilerParams(collective_id=0, has_side_effects=True, vmem_limit_bytes=32 * 2**20),
        )(*(pltpu.with_memory_space_constraint(a, pltpu.HBM) for a in (q, k, v)))

    return jax.shard_map(
        step,
        mesh=mesh,
        in_specs=(P("dp", None, None), P("dp", "sp", None, None), P("dp", "sp", None, None)),
        out_specs=P("dp", None, None),
        check_vma=False,
    )
```

```python
import functools

import jax
import jax.numpy as jnp
from jax import lax
from jax.experimental import pallas as pl
from jax.experimental.pallas import tpu as pltpu
from jax.sharding import PartitionSpec as P

SLOTS = 4
AHEAD = 6
TILE = 4
LOG2E = 1.4426950408889634
MESH = pl.DeviceIdType.MESH
dma = pltpu.SemaphoreType.DMA


def kernel(n, q_hbm, k_hbm, v_hbm, o_ref, qv, kbuf, vbuf, sbuf, wbuf, parts, stats, part_send, part_recv, stat_send, stat_recv):
    seqs, heads, head = q_hbm.shape
    kv_heads = k_hbm.shape[1]
    rep = heads // kv_heads
    pairs = kv_heads // 2
    rows = 2 * rep
    half = head // 2
    wide = half // TILE
    last = seqs - 1
    tiles = seqs // TILE
    old = tiles // 2
    ahead = pairs - 2
    early = ahead * rows
    scale = head**-0.5 * LOG2E
    me = lax.axis_index("sp")
    groups = ((0, old * TILE), (old * TILE, last - TILE + 1), (last - TILE + 1, last))

    first = lax.broadcasted_iota(jnp.int32, (rows, head), 0) < rep
    lane = lax.broadcasted_iota(jnp.int32, (rows, head), 1)

    def scores(b):
        q = qv[b].astype(jnp.float32)
        for p in range(pairs):
            x = q[p * rows : (p + 1) * rows]
            both = jnp.concatenate([jnp.where(first, x, 0.0), jnp.where(first, 0.0, x)], 1).astype(jnp.bfloat16)
            slot = lax.rem(b, SLOTS)
            keys = jnp.concatenate([kbuf[slot, 2 * p], kbuf[slot, 2 * p + 1]], 1)
            sbuf[lax.rem(b, 2), p] = lax.dot_general(both, keys, (((1,), (1,)), ((), ())), preferred_element_type=jnp.float32)

    def weights(b):
        tile = b // TILE
        at = lax.rem(b, TILE) * wide
        stat = stats[me, tile]
        for p in range(pairs):
            s = sbuf[lax.rem(b, 2), p] * scale
            high = jnp.max(s, 1, keepdims=True)
            w = jnp.exp2(s - high)
            total = jnp.sum(w, 1, keepdims=True)
            stat = jnp.where(lane == at + p, high, stat)
            stat = jnp.where(lane == half + at + p, total, stat)
            wbuf[lax.rem(b, AHEAD + 1), p] = w.astype(jnp.bfloat16)
        stats[me, tile] = stat

    def seen(b, p):
        slot = lax.rem(b, SLOTS)
        vals = jnp.concatenate([vbuf[slot, 2 * p], vbuf[slot, 2 * p + 1]], 1)
        out = jnp.dot(wbuf[lax.rem(b, AHEAD + 1), p], vals, preferred_element_type=jnp.float32)
        return jnp.where(first, out[:, :head], out[:, head:])

    def values(b):
        parts[me, b] = jnp.concatenate([seen(b, p) for p in range(pairs)], 0).astype(jnp.bfloat16)

    def to(d):
        return {"sp": lax.rem(me + d, n)}

    peers = sorted(range(1, n), key=lambda d: -min(d, n - d))

    def send(ref, sent, received):
        for d in peers:
            pltpu.make_async_remote_copy(ref, ref, sent.at[0], received, device_id=to(d), device_id_type=MESH).start()

    def send_part(b, g):
        send(parts.at[me, b], part_send, part_recv.at[g])

    def send_stat(t, g):
        send(stats.at[me, t], stat_send, stat_recv.at[g])

    def landed(ref, sem):
        pltpu.make_async_copy(ref, ref, sem).wait()

    others = pl.ds(0, n - 1)

    def shares(t):
        st = [stats[d, t] for d in range(n)]
        top = functools.reduce(jnp.maximum, st)
        w = [jnp.exp2(s - top) for s in st]
        total = sum(a * pltpu.roll(s, half, 1) for a, s in zip(w, st))
        return [a / total for a in w]

    def factors(w, j):
        lanes = [j * wide + p for p in range(pairs)]
        return [[jnp.broadcast_to(a[:, x : x + 1], (rows, head)) for a in w] for x in lanes]

    def mixed(b, ps, f):
        x = [parts[d, b, pl.ds(ps[0] * rows, len(ps) * rows)].astype(jnp.float32) for d in range(n)]
        return jnp.concatenate([sum(f[p][d] * x[d][i * rows : (i + 1) * rows] for d in range(n)) for i, p in enumerate(ps)], 0)

    def combine(t, w, j):
        o_ref[t * TILE + j] = mixed(t * TILE + j, range(pairs), factors(w, j)).astype(o_ref.dtype)

    def combine_tile(t, carry):
        w = shares(t)
        for j in range(TILE):
            combine(t, w, j)
        return carry

    @functools.partial(pl.run_scoped, q_sem=dma, k_sem=dma((SLOTS,)), v_sem=dma((SLOTS,)), end_sem=dma((2,)))
    def _(q_sem, k_sem, v_sem, end_sem):
        def fetch_k(b):
            slot = lax.rem(b, SLOTS)
            return pltpu.make_async_copy(k_hbm.at[b], kbuf.at[slot], k_sem.at[slot])

        def fetch_v(b):
            slot = lax.rem(b, SLOTS)
            return pltpu.make_async_copy(v_hbm.at[b], vbuf.at[slot], v_sem.at[slot])

        def fetch_end(e):
            cut = early // rep
            part = pl.ds(0, cut) if e == 0 else pl.ds(cut, kv_heads - cut)
            return pltpu.make_async_copy(v_hbm.at[last, part], vbuf.at[last % SLOTS, part], end_sem.at[e])

        def fetch_q():
            return pltpu.make_async_copy(q_hbm, qv, q_sem)

        fetch_q().start()
        barrier = pltpu.get_barrier_semaphore()
        for d in range(1, n):
            pl.semaphore_signal(barrier, inc=1, device_id={"sp": lax.rem(me + d, n)}, device_id_type=MESH)
        for b in range(SLOTS):
            fetch_k(b).start()

        def refill_k(b):
            @pl.when(b < seqs)
            def _():
                fetch_k(b).start()

        def refill_v(b):
            @pl.when((b >= 0) & (b < last))
            def _():
                fetch_v(b).start()

            @pl.when(b == last)
            def _():
                for e in range(2):
                    fetch_end(e).start()

        fetch_q().wait()
        fetch_k(0).wait()
        scores(0)
        refill_k(SLOTS)

        def fill(i, carry):
            fetch_k(i).wait()
            weights(i - 1)
            scores(i)
            refill_k(i + SLOTS)
            refill_v(i - AHEAD + SLOTS)
            return carry

        lax.fori_loop(1, AHEAD, fill, 0)
        pl.semaphore_wait(barrier, n - 1)
        send_stat(0, 0)

        def group(b):
            return jnp.where(b < groups[1][0], 0, jnp.where(b < groups[2][0], 1, 2))

        def step(i, carry):
            done = i - AHEAD - 1

            @pl.when(done >= 0)
            def _():
                send_part(done, group(done))

            @pl.when((lax.rem(i, TILE) == 1) & (i >= AHEAD + 1))
            def _():
                t = i // TILE - 1
                send_stat(t, jnp.minimum(group(t * TILE), 1))

            @pl.when(i == groups[0][1] + AHEAD + TILE)
            def _():
                span = pl.ds(0, groups[0][1])
                landed(parts.at[others, span], part_recv.at[0])
                landed(stats.at[others, pl.ds(0, old)], stat_recv.at[0])
                lax.fori_loop(0, old, combine_tile, 0)

            fetch_k(i).wait()
            fetch_v(i - AHEAD).wait()
            values(i - AHEAD)
            weights(i - 1)
            scores(i)
            refill_k(i + SLOTS)
            refill_v(i - AHEAD + SLOTS)
            return carry

        lax.fori_loop(AHEAD, seqs, step, 0)

        weights(last)
        send_stat(tiles - 1, 1)

        def finish(b, carry):
            fetch_v(b).wait()
            send_part(b - 1, group(b - 1))
            values(b)
            refill_v(b + SLOTS)
            return carry

        lax.fori_loop(last - AHEAD + 1, last, finish, 0)

        fetch_end(0).wait()
        send_part(last - 1, 2)
        outs = [seen(last, p) for p in range(ahead)]
        parts[me, last, pl.ds(0, early)] = jnp.concatenate(outs, 0).astype(jnp.bfloat16)
        send(parts.at[me, last, pl.ds(0, early)], part_send, part_recv.at[3])
        fetch_end(1).wait()
        outs = [seen(last, p) for p in range(ahead, pairs)]
        parts[me, last, pl.ds(early, heads - early)] = jnp.concatenate(outs, 0).astype(jnp.bfloat16)
        send(parts.at[me, last, pl.ds(early, heads - early)], part_send, part_recv.at[4])

    landed(parts.at[others, pl.ds(groups[1][0], groups[1][1] - groups[1][0])], part_recv.at[1])
    landed(stats.at[others, pl.ds(old, tiles - old)], stat_recv.at[1])
    lax.fori_loop(old, tiles - 1, combine_tile, 0)
    w = shares(tiles - 1)
    landed(parts.at[others, pl.ds(0, TILE - 1)], part_recv.at[2])
    for j in range(TILE - 1):
        combine(tiles - 1, w, j)
    f = factors(w, TILE - 1)
    landed(parts.at[others, last, pl.ds(0, early)], part_recv.at[3])
    o_ref[last, pl.ds(0, early)] = mixed(last, range(ahead), f).astype(o_ref.dtype)
    landed(parts.at[others], part_send.at[0])
    landed(stats.at[others], stat_send.at[0])
    landed(parts.at[others, last, pl.ds(early, heads - early)], part_recv.at[4])
    o_ref[last, pl.ds(early, heads - early)] = mixed(last, range(ahead, pairs), f).astype(o_ref.dtype)


def solution(mesh):
    n = mesh.shape["sp"]

    def step(q, k, v):
        seqs, heads, head = q.shape
        tokens, kv_heads = k.shape[1:3]
        k, v = (jnp.transpose(a, (0, 2, 1, 3)) for a in (k, v))
        pairs, rows = kv_heads // 2, 2 * heads // kv_heads
        f32, bf16 = jnp.float32, jnp.bfloat16
        return pl.pallas_call(
            functools.partial(kernel, n),
            out_shape=jax.ShapeDtypeStruct(q.shape, q.dtype),
            in_specs=[pl.BlockSpec(memory_space=pl.ANY)] * 3,
            out_specs=pl.BlockSpec(memory_space=pltpu.VMEM),
            scratch_shapes=[
                pltpu.VMEM(q.shape, q.dtype),
                pltpu.VMEM((SLOTS, kv_heads, tokens, head), k.dtype),
                pltpu.VMEM((SLOTS, kv_heads, tokens, head), v.dtype),
                pltpu.VMEM((2, pairs, rows, tokens), f32),
                pltpu.VMEM((AHEAD + 1, pairs, rows, tokens), bf16),
                pltpu.VMEM((n, seqs, heads, head), bf16),
                pltpu.VMEM((n, seqs // TILE, rows, head), f32),
                dma((1,)),
                dma((5,)),
                dma((1,)),
                dma((2,)),
            ],
            compiler_params=pltpu.CompilerParams(collective_id=0, has_side_effects=True, vmem_limit_bytes=32 * 2**20),
        )(*(pltpu.with_memory_space_constraint(a, pltpu.HBM) for a in (q, k, v)))

    return jax.shard_map(
        step,
        mesh=mesh,
        in_specs=(P("dp", None, None), P("dp", "sp", None, None), P("dp", "sp", None, None)),
        out_specs=P("dp", None, None),
        check_vma=False,
    )
```

```python
import functools

import jax
import jax.numpy as jnp
from jax import lax
from jax.experimental import pallas as pl
from jax.experimental.pallas import tpu as pltpu
from jax.sharding import PartitionSpec as P

SLOTS = 4
AHEAD = 6
TILE = 4
LOG2E = 1.4426950408889634
MESH = pl.DeviceIdType.MESH
dma = pltpu.SemaphoreType.DMA


def kernel(n, q_hbm, k_hbm, v_hbm, o_ref, qv, kbuf, vbuf, sbuf, wbuf, parts, stats, part_recv, stat_recv):
    seqs, heads, head = q_hbm.shape
    kv_heads = k_hbm.shape[1]
    rep = heads // kv_heads
    pairs = kv_heads // 2
    rows = 2 * rep
    half = head // 2
    wide = half // TILE
    last = seqs - 1
    tiles = seqs // TILE
    old = tiles // 2
    ahead = pairs - 2
    early = ahead * rows
    scale = head**-0.5 * LOG2E
    me = lax.axis_index("sp")
    groups = ((0, old * TILE), (old * TILE, last - TILE + 1), (last - TILE + 1, last))

    first = lax.broadcasted_iota(jnp.int32, (rows, head), 0) < rep
    lane = lax.broadcasted_iota(jnp.int32, (rows, head), 1)

    def scores(b):
        q = qv[b].astype(jnp.float32)
        for p in range(pairs):
            x = q[p * rows : (p + 1) * rows]
            both = jnp.concatenate([jnp.where(first, x, 0.0), jnp.where(first, 0.0, x)], 1).astype(jnp.bfloat16)
            slot = lax.rem(b, SLOTS)
            keys = jnp.concatenate([kbuf[slot, 2 * p], kbuf[slot, 2 * p + 1]], 1)
            sbuf[lax.rem(b, 2), p] = lax.dot_general(both, keys, (((1,), (1,)), ((), ())), preferred_element_type=jnp.float32)

    def weights(b):
        tile = b // TILE
        at = lax.rem(b, TILE) * wide
        stat = stats[me, tile]
        for p in range(pairs):
            s = sbuf[lax.rem(b, 2), p] * scale
            high = jnp.max(s, 1, keepdims=True)
            w = jnp.exp2(s - high)
            total = jnp.sum(w, 1, keepdims=True)
            stat = jnp.where(lane == at + p, high, stat)
            stat = jnp.where(lane == half + at + p, total, stat)
            wbuf[lax.rem(b, AHEAD + 1), p] = w.astype(jnp.bfloat16)
        stats[me, tile] = stat

    def seen(b, p):
        slot = lax.rem(b, SLOTS)
        vals = jnp.concatenate([vbuf[slot, 2 * p], vbuf[slot, 2 * p + 1]], 1)
        out = jnp.dot(wbuf[lax.rem(b, AHEAD + 1), p], vals, preferred_element_type=jnp.float32)
        return jnp.where(first, out[:, :head], out[:, head:])

    def values(b):
        parts[me, b] = jnp.concatenate([seen(b, p) for p in range(pairs)], 0).astype(jnp.bfloat16)

    def to(d):
        return {"sp": lax.rem(me + d, n)}

    peers = sorted(range(1, n), key=lambda d: -min(d, n - d))

    def send(ref, sent, received):
        for d in peers:
            pltpu.make_async_remote_copy(ref, ref, sent.at[0], received, device_id=to(d), device_id_type=MESH).start()

    def landed(ref, sem):
        pltpu.make_async_copy(ref, ref, sem).wait()

    others = pl.ds(0, n - 1)

    def shares(t):
        st = [stats[d, t] for d in range(n)]
        top = functools.reduce(jnp.maximum, st)
        w = [jnp.exp2(s - top) for s in st]
        total = sum(a * pltpu.roll(s, half, 1) for a, s in zip(w, st))
        return [a / total for a in w]

    def factors(w, j):
        lanes = [j * wide + p for p in range(pairs)]
        return [[jnp.broadcast_to(a[:, x : x + 1], (rows, head)) for a in w] for x in lanes]

    def mixed(b, ps, f):
        x = [parts[d, b, pl.ds(ps[0] * rows, len(ps) * rows)].astype(jnp.float32) for d in range(n)]
        return jnp.concatenate([sum(f[p][d] * x[d][i * rows : (i + 1) * rows] for d in range(n)) for i, p in enumerate(ps)], 0)

    def combine(t, w, j):
        o_ref[t * TILE + j] = mixed(t * TILE + j, range(pairs), factors(w, j)).astype(o_ref.dtype)

    def combine_tile(t, carry):
        w = shares(t)
        for j in range(TILE):
            combine(t, w, j)
        return carry

    @functools.partial(pl.run_scoped, part_send=dma((1,)), stat_send=dma((1,)), q_sem=dma, k_sem=dma((SLOTS,)), v_sem=dma((SLOTS,)), end_sem=dma((2,)))
    def _(part_send, stat_send, q_sem, k_sem, v_sem, end_sem):
        def send_part(b, g):
            send(parts.at[me, b], part_send, part_recv.at[g])

        def send_stat(t, g):
            send(stats.at[me, t], stat_send, stat_recv.at[g])

        def fetch_k(b):
            slot = lax.rem(b, SLOTS)
            return pltpu.make_async_copy(k_hbm.at[b], kbuf.at[slot], k_sem.at[slot])

        def fetch_v(b):
            slot = lax.rem(b, SLOTS)
            return pltpu.make_async_copy(v_hbm.at[b], vbuf.at[slot], v_sem.at[slot])

        def fetch_end(e):
            cut = early // rep
            part = pl.ds(0, cut) if e == 0 else pl.ds(cut, kv_heads - cut)
            return pltpu.make_async_copy(v_hbm.at[last, part], vbuf.at[last % SLOTS, part], end_sem.at[e])

        def fetch_q():
            return pltpu.make_async_copy(q_hbm, qv, q_sem)

        fetch_q().start()
        barrier = pltpu.get_barrier_semaphore()
        for d in range(1, n):
            pl.semaphore_signal(barrier, inc=1, device_id={"sp": lax.rem(me + d, n)}, device_id_type=MESH)
        for b in range(SLOTS):
            fetch_k(b).start()

        def refill_k(b):
            @pl.when(b < seqs)
            def _():
                fetch_k(b).start()

        def refill_v(b):
            @pl.when((b >= 0) & (b < last))
            def _():
                fetch_v(b).start()

            @pl.when(b == last)
            def _():
                for e in range(2):
                    fetch_end(e).start()

        fetch_q().wait()
        fetch_k(0).wait()
        scores(0)
        refill_k(SLOTS)

        def fill(i, carry):
            fetch_k(i).wait()
            weights(i - 1)
            scores(i)
            refill_k(i + SLOTS)
            refill_v(i - AHEAD + SLOTS)
            return carry

        lax.fori_loop(1, AHEAD, fill, 0)
        pl.semaphore_wait(barrier, n - 1)
        send_stat(0, 0)

        def group(b):
            return jnp.where(b < groups[1][0], 0, jnp.where(b < groups[2][0], 1, 2))

        def step(i, carry):
            done = i - AHEAD - 1

            @pl.when(done >= 0)
            def _():
                send_part(done, group(done))

            @pl.when((lax.rem(i, TILE) == 1) & (i >= AHEAD + 1))
            def _():
                t = i // TILE - 1
                send_stat(t, jnp.minimum(group(t * TILE), 1))

            @pl.when(i == groups[0][1] + AHEAD + TILE)
            def _():
                span = pl.ds(0, groups[0][1])
                landed(parts.at[others, span], part_recv.at[0])
                landed(stats.at[others, pl.ds(0, old)], stat_recv.at[0])
                lax.fori_loop(0, old, combine_tile, 0)

            fetch_k(i).wait()
            fetch_v(i - AHEAD).wait()
            values(i - AHEAD)
            weights(i - 1)
            scores(i)
            refill_k(i + SLOTS)
            refill_v(i - AHEAD + SLOTS)
            return carry

        lax.fori_loop(AHEAD, seqs, step, 0)

        weights(last)
        send_stat(tiles - 1, 1)

        def finish(b, carry):
            fetch_v(b).wait()
            send_part(b - 1, group(b - 1))
            values(b)
            refill_v(b + SLOTS)
            return carry

        lax.fori_loop(last - AHEAD + 1, last, finish, 0)

        fetch_end(0).wait()
        send_part(last - 1, 2)
        outs = [seen(last, p) for p in range(ahead)]
        parts[me, last, pl.ds(0, early)] = jnp.concatenate(outs, 0).astype(jnp.bfloat16)
        send(parts.at[me, last, pl.ds(0, early)], part_send, part_recv.at[3])
        fetch_end(1).wait()
        outs = [seen(last, p) for p in range(ahead, pairs)]
        parts[me, last, pl.ds(early, heads - early)] = jnp.concatenate(outs, 0).astype(jnp.bfloat16)
        send(parts.at[me, last, pl.ds(early, heads - early)], part_send, part_recv.at[4])
        landed(parts.at[others], part_send.at[0])
        landed(stats.at[others], stat_send.at[0])

    landed(parts.at[others, pl.ds(groups[1][0], groups[1][1] - groups[1][0])], part_recv.at[1])
    landed(stats.at[others, pl.ds(old, tiles - old)], stat_recv.at[1])
    lax.fori_loop(old, tiles - 1, combine_tile, 0)
    w = shares(tiles - 1)
    landed(parts.at[others, pl.ds(0, TILE - 1)], part_recv.at[2])
    for j in range(TILE - 1):
        combine(tiles - 1, w, j)
    f = factors(w, TILE - 1)
    landed(parts.at[others, last, pl.ds(0, early)], part_recv.at[3])
    o_ref[last, pl.ds(0, early)] = mixed(last, range(ahead), f).astype(o_ref.dtype)
    landed(parts.at[others, last, pl.ds(early, heads - early)], part_recv.at[4])
    o_ref[last, pl.ds(early, heads - early)] = mixed(last, range(ahead, pairs), f).astype(o_ref.dtype)


def solution(mesh):
    n = mesh.shape["sp"]

    def step(q, k, v):
        seqs, heads, head = q.shape
        tokens, kv_heads = k.shape[1:3]
        k, v = (jnp.transpose(a, (0, 2, 1, 3)) for a in (k, v))
        pairs, rows = kv_heads // 2, 2 * heads // kv_heads
        f32, bf16 = jnp.float32, jnp.bfloat16
        return pl.pallas_call(
            functools.partial(kernel, n),
            out_shape=jax.ShapeDtypeStruct(q.shape, q.dtype),
            in_specs=[pl.BlockSpec(memory_space=pl.ANY)] * 3,
            out_specs=pl.BlockSpec(memory_space=pltpu.VMEM),
            scratch_shapes=[
                pltpu.VMEM(q.shape, q.dtype),
                pltpu.VMEM((SLOTS, kv_heads, tokens, head), k.dtype),
                pltpu.VMEM((SLOTS, kv_heads, tokens, head), v.dtype),
                pltpu.VMEM((2, pairs, rows, tokens), f32),
                pltpu.VMEM((AHEAD + 1, pairs, rows, tokens), bf16),
                pltpu.VMEM((n, seqs, heads, head), bf16),
                pltpu.VMEM((n, seqs // TILE, rows, head), f32),
                dma((5,)),
                dma((2,)),
            ],
            compiler_params=pltpu.CompilerParams(collective_id=0, has_side_effects=True, vmem_limit_bytes=32 * 2**20),
        )(*(pltpu.with_memory_space_constraint(a, pltpu.HBM) for a in (q, k, v)))

    return jax.shard_map(
        step,
        mesh=mesh,
        in_specs=(P("dp", None, None), P("dp", "sp", None, None), P("dp", "sp", None, None)),
        out_specs=P("dp", None, None),
        check_vma=False,
    )
```
